256 devices in a mesh: row: 32 (over z, y), col: 8 (over x, core).
Axes of the slice: x: 4, y: 4, z: 8, core: 2. Of those that a mesh axis runs over, the one named last changes fastest.
Arguments:
- tile_seeds: int32 [8, 32, 32, 8], P(None, 'row', None, 'col'), may hold values from 0 to 1073741823
- factors: bfloat16 [8, 4096, 32, 1024], P(None, 'row', None, 'col'), may hold values from -0.015625 to 0.015625
- lower_inverse: bfloat16 [4, 8, 1024, 2, 4096], P(None, None, 'col', None, 'row'), may hold values from -0.1 to 2
- upper_inverse: bfloat16 [4, 8, 1024, 2, 4096], P(None, None, 'col', None, 'row'), may hold values from -0.1 to 2
- right_side: float32 [8, 4096], P(None, 'row'), may hold values from -6 to 6
- first_guess: float32 [32, 1024], P(None, 'col'), may hold values from -6 to 6
Outputs:
- solution: float32 [32, 1024], P(None, 'col')
- hessenberg: float32 [4, 3], replicated
The draws below stay inside these ranges and needn't reach their ends.
All inputs are finite; a program needn't handle non-finite values.
Results may differ from the reference program's by a relative error of at most 0.011.
Values may be sent and summed in bfloat16 or wider, within the bound.
A program may use at most 128 MiB of HBM per device.

```python
import jax
import jax.numpy as jnp
from jax import lax

ORDER = 32768
TILE = 128
SWEEPS = 4
ITERS = 3
DIAG_ORDER = 8192
N_ROW = 32
N_COL = 8


def inverse_blocks(key):
    diag_key, coupling_key = jax.random.split(key)
    shape = (SWEEPS, DIAG_ORDER, DIAG_ORDER)
    diagonal = jax.random.uniform(diag_key, (SWEEPS, DIAG_ORDER), jnp.float32, 0.6, 1.4)
    coupling = jax.random.truncated_normal(coupling_key, -4.0, 4.0, shape, jnp.float32) * (0.3 * DIAG_ORDER ** (-0.5))
    identity_mask = jnp.eye(DIAG_ORDER, dtype=bool)
    blocks = jnp.where(identity_mask[None], diagonal[:, :, None], coupling)
    return blocks.reshape(SWEEPS, DIAG_ORDER // (TILE * N_COL), TILE * N_COL, DIAG_ORDER // (TILE * N_ROW), TILE * N_ROW).astype(jnp.bfloat16)


def draw_lower_inverse(key, part):
    return inverse_blocks(jax.random.fold_in(key, 11))


def draw_upper_inverse(key, part):
    return inverse_blocks(jax.random.fold_in(key, 23))


def set_ends(values, rng, least, largest):
    place = [jax.random.randint(jax.random.fold_in(rng, axis), (), 0, length) for axis, length in enumerate(values.shape)]
    widest = values.shape.index(max(values.shape))
    beside = place[:widest] + [(place[widest] + 1) % values.shape[widest]] + place[widest + 1:]
    return values.at[tuple(place)].set(least).at[tuple(beside)].set(largest)


def block_levels(key, shape, shards, least, top_value):
    def one(axis_at, shards_of):
        draws = jax.random.uniform(jax.random.fold_in(jax.random.fold_in(key, 6), axis_at), (shards_of,), jnp.float32, least / len(shards), top_value / len(shards))
        return jnp.repeat(jnp.exp(draws), shape[axis_at] // shards_of).reshape((-1,) + (1,) * (len(shape) - axis_at - 1))

    loudness = one(*shards[0])
    for cut in shards[1:]:
        loudness = loudness * one(*cut)
    return loudness


def normal_values(rng, shape, width, most, shards=(), kind=jnp.bfloat16):
    result = jax.random.normal(rng, shape, jnp.float32) * width
    if len(shards) > 0:
        result = block_levels(rng, shape, shards, -0.22, 0.18) * result
    return jnp.clip(result, min=-most, max=most).astype(kind)


def setup_inputs(seed: int = 0) -> dict:
    arg_keys = jax.random.split(jax.random.key(seed), 7)
    return {
        "tile_seeds": set_ends(jax.random.randint(arg_keys[0], (ORDER // (TILE * N_ROW), N_ROW, ORDER // (TILE * N_COL), N_COL), 0, 1073741824), jax.random.fold_in(arg_keys[0], 1), 0, 1073741823).astype(jnp.int32),
        "factors": normal_values(arg_keys[1], (ORDER // (TILE * N_ROW), TILE * N_ROW, ORDER // (TILE * N_COL), TILE * N_COL), (4 * ORDER) ** -0.5, 0.015625, ((1, 32), (3, 8))),
        "lower_inverse": draw_lower_inverse(jax.random.fold_in(arg_keys[6], 71), 0),
        "upper_inverse": draw_upper_inverse(jax.random.fold_in(arg_keys[6], 71), 0),
        "right_side": normal_values(arg_keys[4], (ORDER // (TILE * N_ROW), TILE * N_ROW), 1.0, 6.0, ((1, 32),), jnp.float32),
        "first_guess": normal_values(arg_keys[5], (ORDER // (TILE * N_COL), TILE * N_COL), 0.5, 6.0, ((1, 8),), jnp.float32),
    }


DIAG_SHIFT = 2.0

def scrambled(tile_seed, flat_index):
    hashed = tile_seed + flat_index * 1640531527
    hashed = hashed ^ hashed >> 16 & 65535
    hashed = hashed * 2146121005
    hashed = hashed ^ hashed >> 15 & 131071
    hashed = hashed * 1779033703
    hashed = hashed ^ hashed >> 16 & 65535
    high_bits = hashed >> 8 & 16777215
    return (high_bits.astype(jnp.float32) - 8388607.5) / 8388608.0

def small_solve(normal_matrix, target):
    factor = jnp.linalg.cholesky(normal_matrix)
    order_small = normal_matrix.shape[0]
    forward = []
    for position in range(order_small):
        partial_value = target[position]
        for earlier in range(position):
            partial_value = partial_value - factor[position, earlier] * forward[earlier]
        forward.append(partial_value / factor[position, position])
    backward = [None] * order_small
    for position in reversed(range(order_small)):
        partial_value = forward[position]
        for after_pos in range(position + 1, order_small):
            partial_value = partial_value - factor[after_pos, position] * backward[after_pos]
        backward[position] = partial_value / factor[position, position]
    return backward

def matrix_times(seed_grid, vector):
    tile_count = ORDER // TILE
    offsets = jnp.arange(TILE, dtype=jnp.int32)
    flat_index = offsets[:, None] * TILE + offsets[None, :]
    shaped = vector.reshape(tile_count, TILE)
    entry_scale = ORDER ** (-0.5)

    def one_row(seed_row):
        values = scrambled(seed_row[None, :, None], flat_index[:, None, :]) * entry_scale
        return jnp.einsum('icj,cj->i', values, shaped, precision=lax.Precision.HIGHEST)
    return lax.map(one_row, seed_grid).reshape(ORDER) + DIAG_SHIFT * vector

def lower_sweep(matrix, lower_blocks, vector):
    solved = []
    for sweep_step in range(SWEEPS):
        first_row = sweep_step * DIAG_ORDER
        target = vector[first_row:first_row + DIAG_ORDER]
        if sweep_step > 0:
            earlier = jnp.concatenate(solved).astype(jnp.bfloat16)
            target = target - jnp.dot(matrix[first_row:first_row + DIAG_ORDER, :first_row].astype(jnp.float32), earlier.astype(jnp.float32), preferred_element_type=jnp.float32)
        solved.append(jnp.dot(lower_blocks[sweep_step].astype(jnp.float32), target.astype(jnp.bfloat16).astype(jnp.float32), preferred_element_type=jnp.float32))
    return jnp.concatenate(solved)

def upper_sweep(matrix, upper_blocks, vector):
    solved = [None] * SWEEPS
    for sweep_step in reversed(range(SWEEPS)):
        first_row = sweep_step * DIAG_ORDER
        next_row = first_row + DIAG_ORDER
        target = vector[first_row:next_row]
        if sweep_step < SWEEPS - 1:
            later_part = jnp.concatenate(solved[sweep_step + 1:]).astype(jnp.bfloat16)
            target = target - jnp.dot(matrix[first_row:next_row, next_row:].astype(jnp.float32), later_part.astype(jnp.float32), preferred_element_type=jnp.float32)
        solved[sweep_step] = jnp.dot(upper_blocks[sweep_step].astype(jnp.float32), target.astype(jnp.bfloat16).astype(jnp.float32), preferred_element_type=jnp.float32)
    return jnp.concatenate(solved)

def reference(tile_seeds, factors, lower_inverse, upper_inverse, right_side, first_guess):
    tile_count = ORDER // TILE
    seed_grid = tile_seeds.reshape(tile_count, tile_count)
    matrix = factors.reshape(ORDER, ORDER)
    lower_blocks = lower_inverse.reshape(SWEEPS, DIAG_ORDER, DIAG_ORDER)
    upper_blocks = upper_inverse.reshape(SWEEPS, DIAG_ORDER, DIAG_ORDER)
    start_point = first_guess.reshape(ORDER)
    residual = right_side.reshape(ORDER) - matrix_times(seed_grid, start_point)
    initial_norm = jnp.sqrt(jnp.sum(residual * residual))
    basis_list = [residual / initial_norm]
    directions = []
    hessenberg = jnp.zeros((ITERS + 1, ITERS), jnp.float32)
    for column in range(ITERS):
        lowered = lower_sweep(matrix, lower_blocks, basis_list[column])
        direction = upper_sweep(matrix, upper_blocks, lowered)
        directions.append(direction)
        mapped = matrix_times(seed_grid, direction)
        coeffs = jnp.stack([jnp.sum(vector * mapped) for vector in basis_list])
        for position in range(column + 1):
            mapped = mapped - coeffs[position] * basis_list[position]
        length = jnp.sqrt(jnp.sum(mapped * mapped))
        hessenberg = hessenberg.at[:column + 1, column].set(coeffs).at[column + 1, column].set(length)
        if column + 1 < ITERS:
            basis_list.append(mapped / length)
    normal_matrix = jnp.dot(hessenberg.T, hessenberg, precision=lax.Precision.HIGHEST)
    weights = small_solve(normal_matrix, initial_norm * hessenberg[0])
    solution = start_point
    for position in range(ITERS):
        solution = solution + weights[position] * directions[position]
    return (solution.reshape(ORDER // (TILE * N_COL), TILE * N_COL), hessenberg)
```

```python
import functools

import jax
import jax.numpy as jnp
from jax import lax
from jax.experimental import pallas as pl
from jax.experimental.pallas import tpu as pltpu
from jax.sharding import PartitionSpec as P

ORDER = 32768
SWEEPS = 4
ITERS = 3
TILE = 128
N_Z, N_Y = 8, 4
N_ROW, N_COL = 32, 8
DIAG_SHIFT = 2.0
MESH = pl.DeviceIdType.MESH
F32, BF16 = jnp.float32, jnp.bfloat16
SCALE = ORDER ** (-0.5)


def row_peers(r, c):
    z, y = r // N_Y, r % N_Y
    far = lambda d, n: min(d, n - d)
    steps = sorted(range(1, N_ROW), key=lambda d: -far(d // N_Y, N_Z) - far(d % N_Y, N_Y))
    return [(lax.rem(z + d // N_Y, N_Z) * N_Y + lax.rem(y + d % N_Y, N_Y), c) for d in steps]


def col_peers(r, c):
    x, core = c // 2, c % 2
    return [(r, lax.rem(x + d // 2, 4) * 2 + lax.rem(core + d % 2, 2)) for d in (5, 4, 3, 7, 2, 6, 1)]


def send(slot, peers, send_sem, recv_sem):
    for peer in peers:
        pltpu.make_async_remote_copy(
            src_ref=slot, dst_ref=slot, send_sem=send_sem, recv_sem=recv_sem,
            device_id=peer, device_id_type=MESH,
        ).start()


def wait_bytes(ref, sem):
    pltpu.make_async_copy(ref, ref, sem).wait()


def spread(value, first, count):
    rows = [jnp.broadcast_to(value[first + n : first + n + 1, :], (8, TILE)) for n in range(count)]
    return jnp.concatenate(rows, axis=1).astype(BF16)


def fold(wide, count):
    sub = lax.broadcasted_iota(jnp.int32, (8, TILE), 0)
    out = wide[:, :TILE]
    for n in range(1, count):
        out = jnp.where(sub == n, wide[:, n * TILE : (n + 1) * TILE], out)
    return out[:count]


def dot_nt(a, b):
    return lax.dot_general(a, b, (((1,), (1,)), ((), ())), preferred_element_type=F32)


def dot_nn(a, b):
    return lax.dot_general(a, b, (((1,), (0,)), ((), ())), preferred_element_type=F32)


def kernel(
    seeds, f_hbm, li_hbm, ui_hbm, b_ref, x0_ref, x_out, h_out,
    f_raw, i_raw, stage, fw, lw, uw, aw, base, racc, wacc, cacc, yz, zs, vs, u_ref, coef, alpha,
    ybuf, cbuf, wbuf, dbuf, tbuf, dsum,
    in_sem, y_ssem, c_ssem, w_ssem, d_ssem, t_ssem, y_rsem, c_rsem, w_rsem, d_rsem, t_rsem,
):
    r = lax.axis_index("row")
    c = lax.axis_index("col")
    rows_of, cols_of = row_peers(r, c), col_peers(r, c)
    barrier = pltpu.get_barrier_semaphore()
    for peer in rows_of + cols_of:
        pl.semaphore_signal(barrier, inc=1, device_id=peer, device_id_type=MESH)
    f_copy = pltpu.make_async_copy(f_hbm, f_raw, in_sem.at[0])
    l_copy = pltpu.make_async_copy(li_hbm, i_raw.at[0], in_sem.at[1])
    u_copy = pltpu.make_async_copy(ui_hbm, i_raw.at[1], in_sem.at[2])
    f_copy.start()
    l_copy.start()
    u_copy.start()

    own = c == lax.rem(r, N_COL)
    quarter = r // N_COL

    col_id = lax.broadcasted_iota(jnp.int32, (TILE, TILE), 0)
    row_id = lax.broadcasted_iota(jnp.int32, (TILE, TILE), 1)
    base[...] = (row_id * TILE + col_id) * 1640531527
    racc[...] = jnp.zeros_like(racc)

    def make(tc, _):
        x_row = jnp.broadcast_to(x0_ref[pl.ds(tc, 1), :], (TILE, TILE))
        x_col = jnp.sum(jnp.where(col_id == row_id, x_row, 0.0), axis=1, keepdims=True)
        x_all = jnp.broadcast_to(x_col, (TILE, TILE))
        for tr in range(8):
            h = base[...] + seeds[tr, tc]
            h = h ^ lax.shift_right_logical(h, 16)
            h = h * 2146121005
            h = h ^ lax.shift_right_logical(h, 15)
            h = h * 1779033703
            h = h ^ lax.shift_right_logical(h, 16)
            g = (lax.shift_right_logical(h, 8).astype(F32) - 8388607.5) * (SCALE / 8388608.0)
            aw[pl.ds(tc * TILE, TILE), tr * TILE : (tr + 1) * TILE] = g.astype(BF16)
            racc[tr] += jnp.sum((g * x_all).reshape(16, 8, TILE), axis=0)
        return 0

    lax.fori_loop(0, 32, make, 0)

    f_copy.wait()

    def lay_factor(q, _):
        stage[...] = f_raw[q].astype(F32).reshape(TILE * 32, TILE)
        for n in range(32):
            part = stage[pl.ds(n, TILE, stride=32), :]
            fw[pl.ds(q * TILE, TILE), n * TILE : (n + 1) * TILE] = part.astype(BF16)
        return 0

    lax.fori_loop(0, 8, lay_factor, 0)
    l_copy.wait()
    u_copy.wait()
    for which, target in ((0, lw), (1, uw)):

        def lay_inverse(k, _):
            stage[pl.ds(0, 2048), :] = i_raw[which, pl.ds(k * 2048, 2048), :].astype(F32)
            for m in range(2):
                target[k, :, m * TILE : (m + 1) * TILE] = stage[pl.ds(m, 1024, stride=2), :].astype(BF16)
            return 0

        lax.fori_loop(0, SWEEPS, lay_inverse, 0)

    pl.semaphore_wait(barrier, len(rows_of) + len(cols_of))

    def own_rows(ref):
        return ref[pl.ds(quarter, 8, stride=4), :]

    def exchange_w(index, partial):
        wbuf[index, c] = partial
        send(wbuf.at[index, c], cols_of, w_ssem, w_rsem.at[index])
        wait_bytes(wbuf.at[index, pl.ds(0, N_COL - 1)], w_rsem.at[index])
        return jnp.sum(wbuf[index], axis=0)

    def send_dots(index):
        u = u_ref[...]
        for j in range(ITERS):
            dsum[j : j + 1, :] = jnp.sum(vs[j] * u, axis=0, keepdims=True)
        dsum[3:4, :] = jnp.sum(u * u, axis=0, keepdims=True)
        dbuf[index, r] = dsum[...]
        send(dbuf.at[index, r], rows_of, d_ssem, d_rsem.at[index])

    def finish_dots(index):
        wait_bytes(dbuf.at[index, pl.ds(0, N_ROW - 1)], d_rsem.at[index])
        total = jnp.sum(jnp.sum(dbuf[index], axis=0), axis=1, keepdims=True)
        total = jnp.broadcast_to(total, (4, TILE))
        h = [jnp.broadcast_to(total[j : j + 1, :], (8, TILE)) for j in range(4)]
        norm = jnp.sqrt(h[3] - h[0] * h[0] - h[1] * h[1] - h[2] * h[2])
        for j in range(ITERS):
            coef[index, j] = h[j]
        coef[index, 3] = norm
        coef[index, 4] = alpha[...]

    w0 = jnp.concatenate([jnp.sum(racc[tr], axis=0, keepdims=True) for tr in range(8)], axis=0)
    w0 = w0 + jnp.where(own, DIAG_SHIFT * own_rows(x0_ref), 0.0)
    u_ref[...] = b_ref[...] - exchange_w(0, w0)
    vs[...] = jnp.zeros_like(vs)
    zs[...] = jnp.zeros_like(zs)
    alpha[...] = jnp.full((8, TILE), DIAG_SHIFT, F32)

    def iterate(it, _):
        def solve_send(step, weights, target):
            rhs = spread(target, 0, 2)
            part = fold(dot_nt(rhs, weights), 8)
            ybuf[it, step, r] = part.astype(BF16)
            send(ybuf.at[it, step, r], rows_of, y_ssem, y_rsem.at[it, step])

        def solve_wait(step):
            wait_bytes(ybuf.at[it, step, pl.ds(0, N_ROW - 1)], y_rsem.at[it, step])
            return jnp.sum(ybuf[it, step].astype(F32), axis=0)

        def couple_send(step, value):
            cbuf[it, step, c] = value
            send(cbuf.at[it, step, c], cols_of, c_ssem, c_rsem.at[it, step])

        def couple_wait(step):
            wait_bytes(cbuf.at[it, step, pl.ds(0, N_COL - 1)], c_rsem.at[it, step])
            return jnp.sum(cbuf[it, step], axis=0)

        def factor(k, j):
            return fw[k * 256 : (k + 1) * 256, j * 1024 : (j + 1) * 1024]

        for k in range(SWEEPS):
            target = u_ref[2 * k : 2 * k + 2, :]
            if k > 0:
                target = target - couple_wait(k - 1)
            solve_send(k, lw[k], target)
            if k == 0:
                send_dots(it)
            if k == 1:
                finish_dots(it)
                u = u_ref[...]
                for j in range(ITERS):
                    u = u - coef[it, j] * vs[j]
                vs[it] = u / coef[it, 3]
                last = coef[it, 0]
                last = jnp.where(it == 2, coef[it, 1], last)
                alpha[...] = alpha[...] + last
            y = solve_wait(k)
            yz[8 * k : 8 * k + 8, :] = y
            if k < SWEEPS - 1:
                lhs = spread(y, 0, 8)
                out = dot_nt(lhs, factor(k + 1, k))
                if k > 0:
                    out = out + cacc[k + 1]
                couple_send(k, fold(out, 2))
                for i in range(k + 2, SWEEPS):
                    out = dot_nt(lhs, factor(i, k))
                    cacc[i] = out if k == 0 else cacc[i] + out

        @pl.when(own)
        def _():
            tbuf[it] = own_rows(yz)
            send(tbuf.at[it], cols_of, t_ssem, t_rsem)
            wait_bytes(wbuf.at[0, pl.ds(0, N_COL - 1)], t_ssem)

        @pl.when(jnp.logical_not(own))
        def _():
            wait_bytes(tbuf.at[it], t_rsem)

        norm = coef[it, 3]
        for k in reversed(range(SWEEPS)):
            target = tbuf[it, 2 * k : 2 * k + 2, :]
            if k < SWEEPS - 1:
                target = target - couple_wait(SWEEPS - 1 + k)
            solve_send(SWEEPS + k, uw[k], target)
            raw = solve_wait(SWEEPS + k)
            if k > 0:
                lhs = spread(raw, 0, 8)
                out = dot_nt(lhs, factor(k - 1, k))
                if k < SWEEPS - 1:
                    out = out + cacc[k - 1]
                couple_send(SWEEPS - 1 + k - 1, fold(out, 2))
                for i in range(k - 1):
                    out = dot_nt(lhs, factor(i, k))
                    cacc[i] = out if k == SWEEPS - 1 else cacc[i] + out
            z = raw
            for j in range(ITERS):
                z = z - coef[it, j] * zs[j, 8 * k : 8 * k + 8, :]
            z = z / norm
            yz[8 * k : 8 * k + 8, :] = z
            lhs = spread(z, 0, 8)
            out = dot_nn(lhs, aw[k * 1024 : (k + 1) * 1024, :])
            wacc[...] = out if k == SWEEPS - 1 else wacc[...] + out
        zs[it] = yz[...]
        w = fold(wacc[...], 8) + jnp.where(own, DIAG_SHIFT * own_rows(yz), 0.0)
        u_ref[...] = exchange_w(it + 1, w) - alpha[...] * vs[it]
        return 0

    lax.fori_loop(0, ITERS, iterate, 0)
    send_dots(ITERS)
    finish_dots(ITERS)

    beta = coef[0, 3]
    zero = jnp.zeros((8, TILE), F32)
    hess = [[zero] * ITERS for _ in range(ITERS + 1)]
    for k in range(ITERS):
        for j in range(k + 1):
            hess[j][k] = coef[k + 1, j] + (coef[k + 1, 4] if j == k else 0.0)
        hess[k + 1][k] = coef[k + 1, 3]
    normal = [[sum(hess[i][a] * hess[i][d] for i in range(ITERS + 1)) for d in range(ITERS)] for a in range(ITERS)]
    rhs = [beta * hess[0][a] for a in range(ITERS)]
    low = [[None] * ITERS for _ in range(ITERS)]
    for a in range(ITERS):
        for d in range(a + 1):
            v = normal[a][d]
            for e in range(d):
                v = v - low[a][e] * low[d][e]
            low[a][d] = jnp.sqrt(v) if a == d else v / low[d][d]
    fwd = []
    for a in range(ITERS):
        v = rhs[a]
        for e in range(a):
            v = v - low[a][e] * fwd[e]
        fwd.append(v / low[a][a])
    wts = [None] * ITERS
    for a in reversed(range(ITERS)):
        v = fwd[a]
        for e in range(a + 1, ITERS):
            v = v - low[e][a] * wts[e]
        wts[a] = v / low[a][a]
    for k in range(SWEEPS):
        part = x0_ref[8 * k : 8 * k + 8, :]
        for a in range(ITERS):
            part = part + wts[a] * zs[a, 8 * k : 8 * k + 8, :]
        x_out[8 * k : 8 * k + 8, :] = part
    sub = lax.broadcasted_iota(jnp.int32, (8, TILE), 0)
    lane = lax.broadcasted_iota(jnp.int32, (8, TILE), 1)
    table = zero
    for j in range(ITERS + 1):
        for k in range(ITERS):
            if j <= k + 1:
                table = jnp.where((sub == j) & (lane == k), hess[j][k], table)
    h_out[...] = table

    def drain(it, _):
        for step in range(2 * SWEEPS):
            wait_bytes(ybuf.at[it, step, pl.ds(0, N_ROW - 1)], y_ssem)
        for step in range(2 * SWEEPS - 2):
            wait_bytes(cbuf.at[it, step, pl.ds(0, N_COL - 1)], c_ssem)
        return 0

    lax.fori_loop(0, ITERS, drain, 0)
    for index in range(ITERS + 1):
        wait_bytes(wbuf.at[index, pl.ds(0, N_COL - 1)], w_ssem)
        wait_bytes(dbuf.at[index, pl.ds(0, N_ROW - 1)], d_ssem)


def shards(tile_seeds, factors, lower_inverse, upper_inverse, right_side, first_guess):
    vmem = pl.BlockSpec(memory_space=pltpu.VMEM)
    hbm = pl.BlockSpec(memory_space=pl.ANY)
    dma = pltpu.SemaphoreType.DMA
    x, h = pl.pallas_call(
        kernel,
        out_shape=(jax.ShapeDtypeStruct((32, TILE), F32), jax.ShapeDtypeStruct((8, TILE), F32)),
        in_specs=[pl.BlockSpec(memory_space=pltpu.SMEM), hbm, hbm, hbm, vmem, vmem],
        out_specs=(vmem, vmem),
        scratch_shapes=[
            pltpu.VMEM((8, TILE, 32, TILE), BF16),
            pltpu.VMEM((2, 8192, TILE), BF16),
            pltpu.VMEM((4096, TILE), F32),
            pltpu.VMEM((1024, 4096), BF16),
            pltpu.VMEM((SWEEPS, 1024, 256), BF16),
            pltpu.VMEM((SWEEPS, 1024, 256), BF16),
            pltpu.VMEM((4096, 1024), BF16),
            pltpu.VMEM((TILE, TILE), jnp.int32),
            pltpu.VMEM((8, 8, TILE), F32),
            pltpu.VMEM((8, 1024), F32),
            pltpu.VMEM((SWEEPS, 8, 256), F32),
            pltpu.VMEM((32, TILE), F32),
            pltpu.VMEM((ITERS, 32, TILE), F32),
            pltpu.VMEM((ITERS, 8, TILE), F32),
            pltpu.VMEM((8, TILE), F32),
            pltpu.VMEM((ITERS + 1, 5, 8, TILE), F32),
            pltpu.VMEM((8, TILE), F32),
            pltpu.VMEM((ITERS, 2 * SWEEPS, N_ROW, 8, TILE), BF16),
            pltpu.VMEM((ITERS, 2 * SWEEPS - 2, N_COL, 2, TILE), F32),
            pltpu.VMEM((ITERS + 1, N_COL, 8, TILE), F32),
            pltpu.VMEM((ITERS + 1, N_ROW, 4, TILE), F32),
            pltpu.VMEM((ITERS, 8, TILE), F32),
            pltpu.VMEM((4, TILE), F32),
            dma((3,)), dma, dma, dma, dma, dma,
            dma((ITERS, 2 * SWEEPS)), dma((ITERS, 2 * SWEEPS - 2)), dma((ITERS + 1,)), dma((ITERS + 1,)), dma,
        ],
        compiler_params=pltpu.CompilerParams(collective_id=0, has_side_effects=True, vmem_limit_bytes=62 << 20),
        name="refine",
    )(
        tile_seeds.reshape(8, 32), factors, lower_inverse.reshape(8192, TILE), upper_inverse.reshape(8192, TILE),
        right_side, first_guess,
    )
    return x, h[: ITERS + 1, :ITERS]


def solution(mesh):
    in_specs = (
        P(None, "row", None, "col"),
        P(None, "row", None, "col"),
        P(None, None, "col", None, "row"),
        P(None, None, "col", None, "row"),
        P(None, "row"),
        P(None, "col"),
    )
    out_specs = (P(None, "col"), P())
    return jax.shard_map(shards, mesh=mesh, in_specs=in_specs, out_specs=out_specs, check_vma=False)
```

```python
import functools

import jax
import jax.numpy as jnp
from jax import lax
from jax.experimental import pallas as pl
from jax.experimental.pallas import tpu as pltpu
from jax.sharding import PartitionSpec as P

ORDER = 32768
SWEEPS = 4
ITERS = 3
TILE = 128
N_Z, N_Y = 8, 4
N_ROW, N_COL = 32, 8
DIAG_SHIFT = 2.0
MESH = pl.DeviceIdType.MESH
F32, BF16 = jnp.float32, jnp.bfloat16
SCALE = ORDER ** (-0.5)


def row_peers(r, c):
    z, y = r // N_Y, r % N_Y
    far = lambda d, n: min(d, n - d)
    steps = sorted(range(1, N_ROW), key=lambda d: -far(d // N_Y, N_Z) - far(d % N_Y, N_Y))
    return [(lax.rem(z + d // N_Y, N_Z) * N_Y + lax.rem(y + d % N_Y, N_Y), c) for d in steps]


def col_peers(r, c):
    x, core = c // 2, c % 2
    return [(r, lax.rem(x + d // 2, 4) * 2 + lax.rem(core + d % 2, 2)) for d in (5, 4, 3, 7, 2, 6, 1)]


def send(slot, peers, send_sem, recv_sem):
    for peer in peers:
        pltpu.make_async_remote_copy(
            src_ref=slot, dst_ref=slot, send_sem=send_sem, recv_sem=recv_sem,
            device_id=peer, device_id_type=MESH,
        ).start()


def wait_bytes(ref, sem):
    pltpu.make_async_copy(ref, ref, sem).wait()


def spread(value, first, count):
    rows = [jnp.broadcast_to(value[first + n : first + n + 1, :], (8, TILE)) for n in range(count)]
    return jnp.concatenate(rows, axis=1).astype(BF16)


def fold(wide, count):
    sub = lax.broadcasted_iota(jnp.int32, (8, TILE), 0)
    out = wide[:, :TILE]
    for n in range(1, count):
        out = jnp.where(sub == n, wide[:, n * TILE : (n + 1) * TILE], out)
    return out[:count]


def dot_nt(a, b):
    return lax.dot_general(a, b, (((1,), (1,)), ((), ())), preferred_element_type=F32)


def dot_nn(a, b):
    return lax.dot_general(a, b, (((1,), (0,)), ((), ())), preferred_element_type=F32)


def kernel(
    seeds, f_hbm, li_hbm, ui_hbm, b_ref, x0_ref, x_out, h_out,
    f_raw, i_raw, stage, fw, lw, uw, aw, base, racc, wacc, cacc, yz, zs, vs, u_ref, coef, alpha,
    ybuf, cbuf, wbuf, dbuf, tbuf, dsum,
    in_sem, y_ssem, c_ssem, w_ssem, d_ssem, t_ssem, y_rsem, c_rsem, w_rsem, d_rsem, t_rsem,
):
    r = lax.axis_index("row")
    c = lax.axis_index("col")
    rows_of, cols_of = row_peers(r, c), col_peers(r, c)
    barrier = pltpu.get_barrier_semaphore()
    for peer in rows_of + cols_of:
        pl.semaphore_signal(barrier, inc=1, device_id=peer, device_id_type=MESH)
    f_copy = pltpu.make_async_copy(f_hbm, f_raw, in_sem.at[0])
    l_copy = pltpu.make_async_copy(li_hbm, i_raw.at[0], in_sem.at[1])
    u_copy = pltpu.make_async_copy(ui_hbm, i_raw.at[1], in_sem.at[2])
    f_copy.start()
    l_copy.start()
    u_copy.start()

    own = c == lax.rem(r, N_COL)
    quarter = r // N_COL

    col_id = lax.broadcasted_iota(jnp.int32, (TILE, TILE), 0)
    row_id = lax.broadcasted_iota(jnp.int32, (TILE, TILE), 1)
    base[...] = (row_id * TILE + col_id) * 1640531527
    racc[...] = jnp.zeros_like(racc)

    def make(tc, _):
        x_row = jnp.broadcast_to(x0_ref[pl.ds(tc, 1), :], (TILE, TILE))
        x_col = jnp.sum(jnp.where(col_id == row_id, x_row, 0.0), axis=1, keepdims=True)
        x_all = jnp.broadcast_to(x_col, (TILE, TILE))
        for tr in range(8):
            h = base[...] + seeds[tr, tc]
            h = h ^ lax.shift_right_logical(h, 16)
            h = h * 2146121005
            h = h ^ lax.shift_right_logical(h, 15)
            h = h * 1779033703
            h = h ^ lax.shift_right_logical(h, 16)
            g = (lax.shift_right_logical(h, 8).astype(F32) - 8388607.5) * (SCALE / 8388608.0)
            aw[pl.ds(tc * TILE, TILE), tr * TILE : (tr + 1) * TILE] = g.astype(BF16)
            racc[tr] += jnp.sum((g * x_all).reshape(16, 8, TILE), axis=0)
        return 0

    lax.fori_loop(0, 32, make, 0)

    def lay_out():
        l_copy.wait()
        u_copy.wait()
        for which, target in ((0, lw), (1, uw)):

            def lay_inverse(k, _):
                stage[pl.ds(0, 2048), :] = i_raw[which, pl.ds(k * 2048, 2048), :].astype(F32)
                for m in range(2):
                    target[k, :, m * TILE : (m + 1) * TILE] = stage[pl.ds(m, 1024, stride=2), :].astype(BF16)
                return 0

            lax.fori_loop(0, SWEEPS, lay_inverse, 0)
        f_copy.wait()

        def lay_factor(q, _):
            for g in range(4):
                rows = f_raw[q, :, 8 * g : 8 * g + 8, :].astype(F32)
                stage[g * 1024 : (g + 1) * 1024, :] = rows.reshape(1024, TILE)
                for n in range(8):
                    part = stage[pl.ds(g * 1024 + n, TILE, stride=8), :]
                    at = (8 * g + n) * TILE
                    fw[pl.ds(q * TILE, TILE), at : at + TILE] = part.astype(BF16)
            return 0

        lax.fori_loop(0, 8, lay_factor, 0)

    pl.semaphore_wait(barrier, len(rows_of) + len(cols_of))

    def own_rows(ref):
        return ref[pl.ds(quarter, 8, stride=4), :]

    def exchange_w(index, partial, between=None):
        wbuf[index, c] = partial
        send(wbuf.at[index, c], cols_of, w_ssem, w_rsem.at[index])
        if between is not None:
            between()
        wait_bytes(wbuf.at[index, pl.ds(0, N_COL - 1)], w_rsem.at[index])
        return jnp.sum(wbuf[index], axis=0)

    def send_dots(index):
        u = u_ref[...]
        for j in range(ITERS):
            dsum[j : j + 1, :] = jnp.sum(vs[j] * u, axis=0, keepdims=True)
        dsum[3:4, :] = jnp.sum(u * u, axis=0, keepdims=True)
        dbuf[index, r] = dsum[...]
        send(dbuf.at[index, r], rows_of, d_ssem, d_rsem.at[index])

    def finish_dots(index):
        wait_bytes(dbuf.at[index, pl.ds(0, N_ROW - 1)], d_rsem.at[index])
        total = jnp.sum(jnp.sum(dbuf[index], axis=0), axis=1, keepdims=True)
        total = jnp.broadcast_to(total, (4, TILE))
        h = [jnp.broadcast_to(total[j : j + 1, :], (8, TILE)) for j in range(4)]
        norm = jnp.sqrt(h[3] - h[0] * h[0] - h[1] * h[1] - h[2] * h[2])
        for j in range(ITERS):
            coef[index, j] = h[j]
        coef[index, 3] = norm
        coef[index, 4] = alpha[...]

    w0 = jnp.concatenate([jnp.sum(racc[tr], axis=0, keepdims=True) for tr in range(8)], axis=0)
    w0 = w0 + jnp.where(own, DIAG_SHIFT * own_rows(x0_ref), 0.0)
    u_ref[...] = b_ref[...] - exchange_w(0, w0, lay_out)
    vs[...] = jnp.zeros_like(vs)
    zs[...] = jnp.zeros_like(zs)
    alpha[...] = jnp.full((8, TILE), DIAG_SHIFT, F32)

    def iterate(it, _):
        def solve_send(step, weights, target):
            rhs = spread(target, 0, 2)
            part = fold(dot_nt(rhs, weights), 8)
            ybuf[it, step, r] = part.astype(BF16)
            send(ybuf.at[it, step, r], rows_of, y_ssem, y_rsem.at[it, step])

        def solve_wait(step):
            wait_bytes(ybuf.at[it, step, pl.ds(0, N_ROW - 1)], y_rsem.at[it, step])
            return jnp.sum(ybuf[it, step].astype(F32), axis=0)

        def couple_send(step, value):
            cbuf[it, step, c] = value
            send(cbuf.at[it, step, c], cols_of, c_ssem, c_rsem.at[it, step])

        def couple_wait(step):
            wait_bytes(cbuf.at[it, step, pl.ds(0, N_COL - 1)], c_rsem.at[it, step])
            return jnp.sum(cbuf[it, step], axis=0)

        def factor(k, j):
            return fw[k * 256 : (k + 1) * 256, j * 1024 : (j + 1) * 1024]

        for k in range(SWEEPS):
            target = u_ref[2 * k : 2 * k + 2, :]
            if k > 0:
                target = target - couple_wait(k - 1)
            solve_send(k, lw[k], target)
            if k == 0:
                send_dots(it)
            if k == 1:
                finish_dots(it)
                u = u_ref[...]
                for j in range(ITERS):
                    u = u - coef[it, j] * vs[j]
                vs[it] = u / coef[it, 3]
                last = coef[it, 0]
                last = jnp.where(it == 2, coef[it, 1], last)
                alpha[...] = alpha[...] + last
            y = solve_wait(k)
            yz[8 * k : 8 * k + 8, :] = y
            if k < SWEEPS - 1:
                lhs = spread(y, 0, 8)
                out = dot_nt(lhs, factor(k + 1, k))
                if k > 0:
                    out = out + cacc[k + 1]
                couple_send(k, fold(out, 2))
                for i in range(k + 2, SWEEPS):
                    out = dot_nt(lhs, factor(i, k))
                    cacc[i] = out if k == 0 else cacc[i] + out

        @pl.when(own)
        def _():
            tbuf[it] = own_rows(yz)
            send(tbuf.at[it], cols_of, t_ssem, t_rsem)
            wait_bytes(wbuf.at[0, pl.ds(0, N_COL - 1)], t_ssem)

        @pl.when(jnp.logical_not(own))
        def _():
            wait_bytes(tbuf.at[it], t_rsem)

        norm = coef[it, 3]
        for k in reversed(range(SWEEPS)):
            target = tbuf[it, 2 * k : 2 * k + 2, :]
            if k < SWEEPS - 1:
                target = target - couple_wait(SWEEPS - 1 + k)
            solve_send(SWEEPS + k, uw[k], target)
            raw = solve_wait(SWEEPS + k)
            if k > 0:
                lhs = spread(raw, 0, 8)
                out = dot_nt(lhs, factor(k - 1, k))
                if k < SWEEPS - 1:
                    out = out + cacc[k - 1]
                couple_send(SWEEPS - 1 + k - 1, fold(out, 2))
                for i in range(k - 1):
                    out = dot_nt(lhs, factor(i, k))
                    cacc[i] = out if k == SWEEPS - 1 else cacc[i] + out
            z = raw
            for j in range(ITERS):
                z = z - coef[it, j] * zs[j, 8 * k : 8 * k + 8, :]
            z = z / norm
            yz[8 * k : 8 * k + 8, :] = z
            lhs = spread(z, 0, 8)
            out = dot_nn(lhs, aw[k * 1024 : (k + 1) * 1024, :])
            wacc[...] = out if k == SWEEPS - 1 else wacc[...] + out
        zs[it] = yz[...]
        w = fold(wacc[...], 8) + jnp.where(own, DIAG_SHIFT * own_rows(yz), 0.0)
        u_ref[...] = exchange_w(it + 1, w) - alpha[...] * vs[it]
        return 0

    lax.fori_loop(0, ITERS, iterate, 0)
    send_dots(ITERS)
    finish_dots(ITERS)

    beta = coef[0, 3]
    zero = jnp.zeros((8, TILE), F32)
    hess = [[zero] * ITERS for _ in range(ITERS + 1)]
    for k in range(ITERS):
        for j in range(k + 1):
            hess[j][k] = coef[k + 1, j] + (coef[k + 1, 4] if j == k else 0.0)
        hess[k + 1][k] = coef[k + 1, 3]
    normal = [[sum(hess[i][a] * hess[i][d] for i in range(ITERS + 1)) for d in range(ITERS)] for a in range(ITERS)]
    rhs = [beta * hess[0][a] for a in range(ITERS)]
    low = [[None] * ITERS for _ in range(ITERS)]
    for a in range(ITERS):
        for d in range(a + 1):
            v = normal[a][d]
            for e in range(d):
                v = v - low[a][e] * low[d][e]
            low[a][d] = jnp.sqrt(v) if a == d else v / low[d][d]
    fwd = []
    for a in range(ITERS):
        v = rhs[a]
        for e in range(a):
            v = v - low[a][e] * fwd[e]
        fwd.append(v / low[a][a])
    wts = [None] * ITERS
    for a in reversed(range(ITERS)):
        v = fwd[a]
        for e in range(a + 1, ITERS):
            v = v - low[e][a] * wts[e]
        wts[a] = v / low[a][a]
    for k in range(SWEEPS):
        part = x0_ref[8 * k : 8 * k + 8, :]
        for a in range(ITERS):
            part = part + wts[a] * zs[a, 8 * k : 8 * k + 8, :]
        x_out[8 * k : 8 * k + 8, :] = part
    sub = lax.broadcasted_iota(jnp.int32, (8, TILE), 0)
    lane = lax.broadcasted_iota(jnp.int32, (8, TILE), 1)
    table = zero
    for j in range(ITERS + 1):
        for k in range(ITERS):
            if j <= k + 1:
                table = jnp.where((sub == j) & (lane == k), hess[j][k], table)
    h_out[...] = table

    def drain(it, _):
        for step in range(2 * SWEEPS):
            wait_bytes(ybuf.at[it, step, pl.ds(0, N_ROW - 1)], y_ssem)
        for step in range(2 * SWEEPS - 2):
            wait_bytes(cbuf.at[it, step, pl.ds(0, N_COL - 1)], c_ssem)
        return 0

    lax.fori_loop(0, ITERS, drain, 0)
    for index in range(ITERS + 1):
        wait_bytes(wbuf.at[index, pl.ds(0, N_COL - 1)], w_ssem)
        wait_bytes(dbuf.at[index, pl.ds(0, N_ROW - 1)], d_ssem)


def shards(tile_seeds, factors, lower_inverse, upper_inverse, right_side, first_guess):
    vmem = pl.BlockSpec(memory_space=pltpu.VMEM)
    hbm = pl.BlockSpec(memory_space=pl.ANY)
    dma = pltpu.SemaphoreType.DMA
    x, h = pl.pallas_call(
        kernel,
        out_shape=(jax.ShapeDtypeStruct((32, TILE), F32), jax.ShapeDtypeStruct((8, TILE), F32)),
        in_specs=[pl.BlockSpec(memory_space=pltpu.SMEM), hbm, hbm, hbm, vmem, vmem],
        out_specs=(vmem, vmem),
        scratch_shapes=[
            pltpu.VMEM((8, TILE, 32, TILE), BF16),
            pltpu.VMEM((2, 8192, TILE), BF16),
            pltpu.VMEM((4096, TILE), F32),
            pltpu.VMEM((1024, 4096), BF16),
            pltpu.VMEM((SWEEPS, 1024, 256), BF16),
            pltpu.VMEM((SWEEPS, 1024, 256), BF16),
            pltpu.VMEM((4096, 1024), BF16),
            pltpu.VMEM((TILE, TILE), jnp.int32),
            pltpu.VMEM((8, 8, TILE), F32),
            pltpu.VMEM((8, 1024), F32),
            pltpu.VMEM((SWEEPS, 8, 256), F32),
            pltpu.VMEM((32, TILE), F32),
            pltpu.VMEM((ITERS, 32, TILE), F32),
            pltpu.VMEM((ITERS, 8, TILE), F32),
            pltpu.VMEM((8, TILE), F32),
            pltpu.VMEM((ITERS + 1, 5, 8, TILE), F32),
            pltpu.VMEM((8, TILE), F32),
            pltpu.VMEM((ITERS, 2 * SWEEPS, N_ROW, 8, TILE), BF16),
            pltpu.VMEM((ITERS, 2 * SWEEPS - 2, N_COL, 2, TILE), F32),
            pltpu.VMEM((ITERS + 1, N_COL, 8, TILE), F32),
            pltpu.VMEM((ITERS + 1, N_ROW, 4, TILE), F32),
            pltpu.VMEM((ITERS, 8, TILE), F32),
            pltpu.VMEM((4, TILE), F32),
            dma((3,)), dma, dma, dma, dma, dma,
            dma((ITERS, 2 * SWEEPS)), dma((ITERS, 2 * SWEEPS - 2)), dma((ITERS + 1,)), dma((ITERS + 1,)), dma,
        ],
        compiler_params=pltpu.CompilerParams(collective_id=0, has_side_effects=True, vmem_limit_bytes=62 << 20),
        name="refine",
    )(
        tile_seeds.reshape(8, 32), factors, lower_inverse.reshape(8192, TILE), upper_inverse.reshape(8192, TILE),
        right_side, first_guess,
    )
    return x, h[: ITERS + 1, :ITERS]


def solution(mesh):
    in_specs = (
        P(None, "row", None, "col"),
        P(None, "row", None, "col"),
        P(None, None, "col", None, "row"),
        P(None, None, "col", None, "row"),
        P(None, "row"),
        P(None, "col"),
    )
    out_specs = (P(None, "col"), P())
    return jax.shard_map(shards, mesh=mesh, in_specs=in_specs, out_specs=out_specs, check_vma=False)
```
